32 devices in a mesh: rows: 4 (over z), cols: 8 (over y, x, core).
Axes of the slice: x: 2, y: 2, z: 4, core: 2. Of those that a mesh axis runs over, the one named last changes fastest.
Arguments:
- features: bfloat16 [12288, 128], P(('rows', 'cols')), may hold values from -6 to 6
- seeds: int32 [384], replicated, may hold values from 0 to 12287
Outputs:
- vector: float32 [12288], P(('rows', 'cols'))
The draws below stay inside these ranges and needn't reach their ends.
All inputs are finite; a program needn't handle non-finite values.
Results may differ from the reference program's by a relative error of at most 0.0013.
Values may be sent and summed in bfloat16 or wider, within the bound.
A program may use at most 128 MiB of HBM per device.

```python
import math
import jax
import jax.numpy as jnp
from jax import lax

D = 128
ITERS = 4
N_POINTS = 12288
SEEDS = 384


def draw_features(key, part):
    key_groups, key_centers, key_noise, key_scale = jax.random.split(key, 4)
    groups = jax.random.randint(key_groups, (N_POINTS,), 0, 256)
    centers = jax.random.normal(key_centers, (256, D), jnp.float32)
    placed = centers[groups]
    points = placed + 0.25 * jax.random.normal(key_noise, (N_POINTS, D), jnp.float32)
    return jnp.clip(points, -6.0, 6.0).astype(jnp.bfloat16)


def set_ends(drawn, own_key, least, top_value):
    dims = drawn.shape
    place = [jax.random.randint(jax.random.fold_in(own_key, axis), (), 0, dims[axis]) for axis in range(len(dims))]
    drawn = drawn.at[tuple(place)].set(least)
    longest = dims.index(max(dims))
    place[longest] = (place[longest] + 1) % dims[longest]
    return drawn.at[tuple(place)].set(top_value)


def setup_inputs(seed: int = 0) -> dict:
    arg_keys = jax.random.split(jax.random.key(seed), 3)
    return {
        "features": draw_features(jax.random.fold_in(arg_keys[2], 71), 0),
        "seeds": set_ends(jax.random.randint(arg_keys[1], (SEEDS,), 0, N_POINTS), jax.random.fold_in(arg_keys[1], 1), 0, N_POINTS - 1).astype(jnp.int32),
    }


def reference(features, seeds):
    total = features.shape[0]
    width = features.shape[1]
    gamma = 4.0 / width
    wide = features.astype(jnp.float32)
    sq = jnp.sum(wide * wide, axis=1)
    block = math.gcd(total, 1024)

    def tile_rows(index):
        start = (index * block).astype(jnp.int32)
        part = lax.dynamic_slice_in_dim(features, start, block, 0)
        part_sq = lax.dynamic_slice_in_dim(sq, start, block, 0)
        gram = lax.dot_general(part, features, (((1,), (1,)), ((), ())), preferred_element_type=jnp.float32)
        dist = part_sq[:, None] + sq[None, :] - 2.0 * gram
        return jnp.exp(-gamma * jnp.maximum(dist, 0.0)).astype(jnp.bfloat16)

    affinity = lax.map(tile_rows, jnp.arange(total // block, dtype=jnp.int32)).reshape(total, total)
    degree = jnp.dot(affinity, jnp.ones((total,), jnp.bfloat16), preferred_element_type=jnp.float32)
    count = jnp.zeros((total,), jnp.float32).at[seeds].add(1.0)
    vector = 1.0 + 32.0 * count
    for step in range(ITERS):
        product = jnp.dot(affinity, vector.astype(jnp.bfloat16), preferred_element_type=jnp.float32)
        scaled = product / degree
        vector = scaled / (jnp.sum(jnp.abs(scaled)) / total)
    return vector
```

```python
import functools

import jax
import jax.numpy as jnp
from jax import lax
from jax.experimental import pallas as pl
from jax.experimental.pallas import tpu as pltpu
from jax.sharding import PartitionSpec as P

ITERS = 4
LANES = 128
MESH = pl.DeviceIdType.MESH


def flip(index, mask):
    bit = 1
    out = index
    while bit <= mask:
        if mask & bit:
            out = out + bit - 2 * bit * ((index // bit) % 2)
        bit *= 2
    return out


def plan(n_rows, n_cols):
    def last_bit(shift, mask):
        if mask & 1:
            return 1
        bits = [1 << k for k in range(n_cols.bit_length()) if mask >> k & 1]
        return bits[shift % len(bits)]

    def key(slot):
        shift, mask = slot
        return 2.1 * shift + 2.1 * bin(mask >> 1).count("1") + 0.5 * (mask & 1)

    slots = sorted(
        ((s, m) for s in range(n_rows) for m in range(n_cols)), key=key
    )
    onward = {slot: [] for slot in slots}
    for shift, mask in slots:
        if mask:
            bit = last_bit(shift, mask)
            onward[(shift, mask ^ bit)].append((bit, (shift, mask)))
    for slot in slots:
        onward[slot].sort(key=lambda item: item[0])
    groups = []
    for at, slot in enumerate(slots):
        if groups and key(slots[groups[-1][0]]) == key(slot) and slot != slots[1]:
            groups[-1].append(at)
        else:
            groups.append([at])
    return slots, onward, groups


def kernel(n_rows, n_cols, feat_ref, seeds_ref, out_ref, feats, weights, lhs, own_sq, seed_rows,
           parts, feat_send, feat_recv, part_send, part_recv):
    seg, width = feat_ref.shape
    slots, onward, groups = plan(n_rows, n_cols)
    at_of = {slot: at for at, slot in enumerate(slots)}
    n_slots = len(slots)
    n_points = n_slots * seg
    gamma = 4.0 / width
    row = lax.axis_index("rows")
    col = lax.axis_index("cols")
    col_bits = [1 << k for k in range(n_cols.bit_length() - 1)]

    def device(shift, mask):
        return ((row + n_rows - shift) % n_rows, flip(col, mask))

    barrier = pltpu.get_barrier_semaphore()
    near = [device(s, 0) for s in range(1, n_rows)] + [device(0, b) for b in col_bits]
    for peer in near:
        pl.semaphore_signal(barrier, inc=1, device_id=peer, device_id_type=MESH)

    own = feat_ref[...]
    wide = own.astype(jnp.float32)
    sq = jnp.sum(wide * wide, axis=1, keepdims=True)
    own_sq[...] = jnp.transpose(jnp.broadcast_to(sq, (seg, LANES)))[:8]
    for q in range(seeds_ref.shape[0]):
        seed_rows[pl.ds(q * LANES, LANES), :] = jnp.transpose(
            jnp.broadcast_to(seeds_ref[q : q + 1, :], (LANES, LANES))
        )
    feats[0] = own
    pl.semaphore_wait(barrier, len(near))

    def hop(source, target_at, peer):
        return pltpu.make_async_remote_copy(
            src_ref=source,
            dst_ref=feats.at[target_at],
            send_sem=feat_send.at[target_at],
            recv_sem=feat_recv.at[target_at],
            device_id=peer,
            device_id_type=MESH,
        )

    sent = []

    def send_on(slot):
        source = feat_ref if slot == (0, 0) else feats.at[at_of[slot]]
        hops = [(device(0, bit), target) for bit, target in onward[slot]]
        if slot == (0, 0):
            hops += [(device(s, 0), (s, 0)) for s in range(1, n_rows)]
        for peer, target in hops:
            copy = hop(source, at_of[target], peer)
            copy.start()
            sent.append(copy)

    def start_row(at):
        shift, mask = slots[at]
        base = (((row + shift) % n_rows) * n_cols + flip(col, mask)) * seg
        for k in range(seg // LANES):
            index = base + k * LANES + lax.broadcasted_iota(jnp.int32, (1, LANES), 1)
            hit = (seed_rows[...] == index).astype(jnp.float32)
            start = 1.0 + 32.0 * jnp.sum(hit, axis=0, keepdims=True)
            first = lax.broadcasted_iota(jnp.int32, (8, LANES), 0) == 0
            lhs[at, :, k * LANES : (k + 1) * LANES] = jnp.where(first, start, 1.0)

    def block(at, total):
        part = feats[at]
        gram = lax.dot_general(
            part, feat_ref[...], (((1,), (1,)), ((), ())), preferred_element_type=jnp.float32
        )
        part_wide = part.astype(jnp.float32)
        part_sq = jnp.sum(part_wide * part_wide, axis=1, keepdims=True)
        dist = part_sq + own_sq[0:1, :] - 2.0 * gram
        value = jnp.exp(-gamma * jnp.maximum(dist, 0.0)).astype(jnp.bfloat16)
        weights[at] = value
        return total + jnp.dot(
            lhs[at].astype(jnp.bfloat16), value, preferred_element_type=jnp.float32
        )

    total = jnp.zeros((8, seg), jnp.float32)
    send_on((0, 0))
    for at in range(n_slots):
        start_row(at)
    for group in groups:
        for at in group:
            if at:
                hop(feat_ref, at, device(0, 1)).wait_recv()
                send_on(slots[at])
        total = lax.fori_loop(group[0], group[-1] + 1, block, total)
    for copy in sent:
        copy.wait_send()

    degree = total[1:2, :]
    product = total[0:1, :]
    step_slots = 4 if n_slots % 4 == 0 else 1
    for step in range(ITERS):
        if step > 0:
            def multiply(at, acc):
                for k in range(step_slots):
                    one = at * step_slots + k
                    row_vec = parts[step - 1, one] / mean
                    left = jnp.broadcast_to(row_vec, (8, seg)).astype(jnp.bfloat16)
                    acc = acc + jnp.dot(left, weights[one], preferred_element_type=jnp.float32)
                return acc

            product = lax.fori_loop(
                0, n_slots // step_slots, multiply, jnp.zeros((8, seg), jnp.float32)
            )[0:1, :]
        scaled = product / degree
        parts[step, 0] = scaled
        for at in range(1, n_slots):
            pltpu.make_async_remote_copy(
                src_ref=parts.at[step, 0],
                dst_ref=parts.at[step, at],
                send_sem=part_send.at[step],
                recv_sem=part_recv.at[step],
                device_id=device(*slots[at]),
                device_id_type=MESH,
            ).start()
        rest = parts.at[step, pl.ds(1, n_slots - 1)]
        pltpu.make_async_copy(rest, rest, part_recv.at[step]).wait()
        mean = jnp.sum(jnp.abs(parts[step])) / n_points
    out_ref[...] = scaled / mean
    for step in range(ITERS):
        rest = parts.at[step, pl.ds(1, n_slots - 1)]
        pltpu.make_async_copy(rest, rest, part_send.at[step]).wait()


def shards(features, seeds):
    n_rows = lax.axis_size("rows")
    n_cols = lax.axis_size("cols")
    seg, width = features.shape
    n_slots = n_rows * n_cols
    pad = -seeds.shape[0] % LANES
    seeds = jnp.pad(seeds, (0, pad), constant_values=-1).reshape(-1, LANES)
    vmem = pl.BlockSpec(memory_space=pltpu.VMEM)
    out = pl.pallas_call(
        functools.partial(kernel, n_rows, n_cols),
        out_shape=jax.ShapeDtypeStruct((1, seg), jnp.float32),
        in_specs=[vmem, vmem],
        out_specs=vmem,
        scratch_shapes=[
            pltpu.VMEM((n_slots, seg, width), jnp.bfloat16),
            pltpu.VMEM((n_slots, seg, seg), jnp.bfloat16),
            pltpu.VMEM((n_slots, 8, seg), jnp.float32),
            pltpu.VMEM((8, seg), jnp.float32),
            pltpu.VMEM((seeds.shape[0] * LANES, LANES), jnp.int32),
            pltpu.VMEM((ITERS, n_slots, 1, seg), jnp.float32),
            pltpu.SemaphoreType.DMA((n_slots,)),
            pltpu.SemaphoreType.DMA((n_slots,)),
            pltpu.SemaphoreType.DMA((ITERS,)),
            pltpu.SemaphoreType.DMA((ITERS,)),
        ],
        compiler_params=pltpu.CompilerParams(
            collective_id=0, has_side_effects=True, vmem_limit_bytes=67043328
        ),
    )(features, seeds)
    return out.reshape(seg)


def solution(mesh):
    in_specs = (P(("rows", "cols"), None), P())
    out_specs = P(("rows", "cols"))
    return jax.shard_map(shards, mesh=mesh, in_specs=in_specs, out_specs=out_specs, check_vma=False)
```

```python
import functools
import math

import jax
import jax.numpy as jnp
from jax import lax
from jax.experimental import pallas as pl
from jax.experimental.pallas import tpu as pltpu
from jax.sharding import PartitionSpec as P

ITERS = 4
LANES = 128
MESH = pl.DeviceIdType.MESH


def flip(index, mask):
    bit = 1
    out = index
    while bit <= mask:
        if mask & bit:
            out = out + bit - 2 * bit * ((index // bit) % 2)
        bit *= 2
    return out


def plan(n_rows, n_cols):
    def last_bit(shift, mask):
        if mask & 1:
            return 1
        bits = [1 << k for k in range(n_cols.bit_length()) if mask >> k & 1]
        return bits[shift % len(bits)]

    def key(slot):
        shift, mask = slot
        return 0.2 * shift + 2.1 * bin(mask >> 1).count("1") + 4.3 * (mask & 1)

    slots = sorted(
        ((s, m) for s in range(n_rows) for m in range(n_cols)), key=key
    )
    onward = {slot: [] for slot in slots}
    for shift, mask in slots:
        if mask:
            bit = last_bit(shift, mask)
            onward[(shift, mask ^ bit)].append((bit, (shift, mask)))
    for slot in slots:
        onward[slot].sort(key=lambda item: item[0])
    size = max(n_rows // 2, 1)
    groups = [[0]] + [
        list(range(at, min(at + size, len(slots)))) for at in range(1, len(slots), size)
    ]
    return slots, onward, groups


def kernel(n_rows, n_cols, feat_ref, seeds_ref, out_ref, feats, weights, lhs, own_scaled, own_sq, seed_rows,
           parts, feat_send, feat_recv, part_send, part_recv):
    seg, width = feat_ref.shape
    slots, onward, groups = plan(n_rows, n_cols)
    at_of = {slot: at for at, slot in enumerate(slots)}
    n_slots = len(slots)
    n_points = n_slots * seg
    gamma = 4.0 / width
    row = lax.axis_index("rows")
    col = lax.axis_index("cols")
    col_bits = [1 << k for k in range(n_cols.bit_length() - 1)]

    def device(shift, mask):
        return ((row + n_rows - shift) % n_rows, flip(col, mask))

    barrier = pltpu.get_barrier_semaphore()
    near = [device(s, 0) for s in range(1, n_rows)] + [device(0, b) for b in col_bits]
    for peer in near:
        pl.semaphore_signal(barrier, inc=1, device_id=peer, device_id_type=MESH)

    own = feat_ref[...]
    wide = own.astype(jnp.float32)
    sq = jnp.sum(wide * wide, axis=1, keepdims=True)
    own_scaled[...] = (wide * (2.0 * gamma)).astype(jnp.bfloat16)
    own_sq[...] = -gamma * jnp.transpose(jnp.broadcast_to(sq, (seg, LANES)))[:8]
    for q in range(seeds_ref.shape[0]):
        seed_rows[pl.ds(q * LANES, LANES), :] = jnp.transpose(
            jnp.broadcast_to(seeds_ref[q : q + 1, :], (LANES, LANES))
        )
    feats[0] = own
    pl.semaphore_wait(barrier, len(near))

    def hop(source, target_at, peer):
        return pltpu.make_async_remote_copy(
            src_ref=source,
            dst_ref=feats.at[target_at],
            send_sem=feat_send.at[target_at],
            recv_sem=feat_recv.at[target_at],
            device_id=peer,
            device_id_type=MESH,
        )

    sent = []

    def send_on(slot):
        source = feat_ref if slot == (0, 0) else feats.at[at_of[slot]]
        hops = [(device(0, bit), target) for bit, target in onward[slot]]
        if slot == (0, 0):
            hops = [(device(s, 0), (s, 0)) for s in range(1, n_rows)] + hops
        for peer, target in hops:
            copy = hop(source, at_of[target], peer)
            copy.start()
            sent.append(copy)

    def start_row(at):
        shift, mask = slots[at]
        base = (((row + shift) % n_rows) * n_cols + flip(col, mask)) * seg
        for k in range(seg // LANES):
            index = base + k * LANES + lax.broadcasted_iota(jnp.int32, (1, LANES), 1)
            hit = (seed_rows[...] == index).astype(jnp.float32)
            start = 1.0 + 32.0 * jnp.sum(hit, axis=0, keepdims=True)
            first = lax.broadcasted_iota(jnp.int32, (8, LANES), 0) == 0
            lhs[at, :, k * LANES : (k + 1) * LANES] = jnp.where(first, start, 1.0)

    def add_product(at, total):
        return total + jnp.dot(
            lhs[at].astype(jnp.bfloat16), weights[at], preferred_element_type=jnp.float32
        )

    def block(at, total, lag):
        if lag:
            total = add_product(at - 1, total)
        for k in range(0, seg, LANES):
            part = feats[at, k : k + LANES, :]
            gram = lax.dot_general(
                part, own_scaled[...], (((1,), (1,)), ((), ())), preferred_element_type=jnp.float32
            )
            part_wide = part.astype(jnp.float32)
            part_sq = -gamma * jnp.sum(part_wide * part_wide, axis=1, keepdims=True)
            exponent = (part_sq + own_sq[0:1, :]) + gram
            weights[at, k : k + LANES, :] = jnp.exp(jnp.minimum(exponent, 0.0)).astype(
                jnp.bfloat16
            )
        return total

    total = jnp.zeros((8, seg), jnp.float32)
    send_on((0, 0))
    for group in groups:
        for at in group:
            if at:
                hop(feat_ref, at, device(0, 1)).wait_recv()
                send_on(slots[at])
        for at in group:
            start_row(at)
        if group[0] == 0:
            total = block(0, total, False)
            group = group[1:]
        if group:
            total = lax.fori_loop(
                group[0], group[-1] + 1, functools.partial(block, lag=True), total
            )
    total = add_product(n_slots - 1, total)
    for copy in sent:
        copy.wait_send()

    degree = total[1:2, :]
    product = total[0:1, :]
    step_slots = math.gcd(n_slots, 8)
    for step in range(ITERS):
        if step > 0:
            def multiply(at, acc):
                left = jnp.concatenate(
                    [parts[step - 1, at * step_slots + k] / mean for k in range(step_slots)], axis=1
                )
                left = jnp.broadcast_to(left, (8, step_slots * seg)).astype(jnp.bfloat16)
                right = weights[pl.ds(at * step_slots, step_slots)].reshape(step_slots * seg, seg)
                return acc + jnp.dot(left, right, preferred_element_type=jnp.float32)

            product = lax.fori_loop(
                0, n_slots // step_slots, multiply, jnp.zeros((8, seg), jnp.float32)
            )[0:1, :]
        scaled = product / degree
        parts[step, 0] = scaled
        for at in range(1, n_slots):
            pltpu.make_async_remote_copy(
                src_ref=parts.at[step, 0],
                dst_ref=parts.at[step, at],
                send_sem=part_send.at[step],
                recv_sem=part_recv.at[step],
                device_id=device(*slots[at]),
                device_id_type=MESH,
            ).start()
        rest = parts.at[step, pl.ds(1, n_slots - 1)]
        pltpu.make_async_copy(rest, rest, part_recv.at[step]).wait()
        mean = jnp.sum(jnp.abs(parts[step])) / n_points
    out_ref[...] = scaled / mean
    for step in range(ITERS):
        rest = parts.at[step, pl.ds(1, n_slots - 1)]
        pltpu.make_async_copy(rest, rest, part_send.at[step]).wait()


def shards(features, seeds):
    n_rows = lax.axis_size("rows")
    n_cols = lax.axis_size("cols")
    seg, width = features.shape
    n_slots = n_rows * n_cols
    pad = -seeds.shape[0] % LANES
    seeds = jnp.pad(seeds, (0, pad), constant_values=-1).reshape(-1, LANES)
    vmem = pl.BlockSpec(memory_space=pltpu.VMEM)
    out = pl.pallas_call(
        functools.partial(kernel, n_rows, n_cols),
        out_shape=jax.ShapeDtypeStruct((1, seg), jnp.float32),
        in_specs=[vmem, vmem],
        out_specs=vmem,
        scratch_shapes=[
            pltpu.VMEM((n_slots, seg, width), jnp.bfloat16),
            pltpu.VMEM((n_slots, seg, seg), jnp.bfloat16),
            pltpu.VMEM((n_slots, 8, seg), jnp.float32),
            pltpu.VMEM((seg, width), jnp.bfloat16),
            pltpu.VMEM((8, seg), jnp.float32),
            pltpu.VMEM((seeds.shape[0] * LANES, LANES), jnp.int32),
            pltpu.VMEM((ITERS, n_slots, 1, seg), jnp.float32),
            pltpu.SemaphoreType.DMA((n_slots,)),
            pltpu.SemaphoreType.DMA((n_slots,)),
            pltpu.SemaphoreType.DMA((ITERS,)),
            pltpu.SemaphoreType.DMA((ITERS,)),
        ],
        compiler_params=pltpu.CompilerParams(
            collective_id=0, has_side_effects=True, vmem_limit_bytes=67043328
        ),
    )(features, seeds)
    return out.reshape(seg)


def solution(mesh):
    in_specs = (P(("rows", "cols"), None), P())
    out_specs = P(("rows", "cols"))
    return jax.shard_map(shards, mesh=mesh, in_specs=in_specs, out_specs=out_specs, check_vma=False)
```
